256 devices in a mesh: grp: 8 (over y, core), shard: 32 (over x, z).
Axes of the slice: x: 4, y: 4, z: 8, core: 2. Of those that a mesh axis runs over, the one named last changes fastest.
Arguments:
- grads: float32 [8, 32, 3456, 512], P('grp', 'shard'), may hold values from -6 to 6
- master: float32 [3456, 512], P('shard'), may hold values from -0.109375 to 0.109375
- moment_one: float32 [3456, 512], P('shard'), may hold values from -0.0004510549 to 0.0004510549
- moment_two: float32 [3456, 512], P('shard'), may hold values from 1.13028066e-10 to 2.8257017e-09
- step_count: int32 [1], replicated, may hold values from 1 to 59
Outputs:
- new_master: float32 [3456, 512], P('shard')
- new_moment_one: float32 [3456, 512], P('shard')
- new_moment_two: float32 [3456, 512], P('shard')
- weights: bfloat16 [3456, 512], replicated
The draws below stay inside these ranges and needn't reach their ends.
All inputs are finite; a program needn't handle non-finite values.
Results may differ from the reference program's by a relative error of at most 0.0004.
Values may be sent and summed in bfloat16 or wider, within the bound.
A program may use at most 128 MiB of HBM per device.

```python
import math
import jax
import jax.numpy as jnp
from jax import lax

IN = 3456
RANK = 512
N_GRP = 8
N_SHARD = 32


def strengthened(drawn, key, source, target, shards_of, factor):
    owner, partner = [(jnp.arange(drawn.shape[dim]) // (drawn.shape[dim] // shards_of)).reshape([-1 if axis == dim else 1 for axis in range(drawn.ndim)]) for dim in (source, target)]
    chosen = jax.random.permutation(key, shards_of)[partner]
    strong = (owner == chosen) | (owner == (partner + shards_of // 2) % shards_of)
    return jnp.where(strong, factor * drawn, drawn)


def shard_levels(key, dims, cuts, least, largest):
    loudness, own = 1.0, jax.random.fold_in(key, 6)
    for position, parts in cuts:
        steps = jnp.exp(jax.random.uniform(jax.random.fold_in(own, position), (parts,), jnp.float32, least / len(cuts), largest / len(cuts)))
        loudness = loudness * jnp.repeat(steps, dims[position] // parts).reshape([-1 if axis == position else 1 for axis in range(len(dims))])
    return loudness


def bell_draw(key, dims, deviation, reach, split=(), kind=jnp.bfloat16):
    result = deviation * jax.random.normal(key, dims, jnp.float32)
    if split:
        result = result * shard_levels(key, dims, split, -0.22, 0.18)
    return jnp.clip(result, -reach, reach).astype(kind)


def heavy_noise(rng, extent, deviation, reach, cuts, heavy, held_as=jnp.bfloat16):
    drawn = deviation * jax.random.normal(rng, extent, jnp.float32)
    if cuts:
        drawn = drawn * shard_levels(rng, extent, cuts, -0.22, 0.18)
    return jnp.clip(strengthened(drawn, jax.random.fold_in(rng, 3), *heavy), -reach, reach).astype(held_as)


def setup_inputs(seed: int = 0) -> dict:
    keys = jax.random.split(jax.random.key(seed), 6)
    grads = heavy_noise(keys[0], (N_GRP, N_SHARD, IN, RANK), 1.0, 6.0, ((0, 8), (1, 32)), (1, 2, 32, 2.75), jnp.float32)
    master = bell_draw(keys[1], (IN, RANK), IN ** -0.5, 0.109375, ((0, 32),), jnp.float32)
    moment_one = bell_draw(keys[2], (IN, RANK), (0.1 * (IN * RANK) ** -0.5), 0.0004510549, ((0, 32),), jnp.float32)
    moment_two = jnp.clip(jnp.exp(math.log(2.8257016726485062e-09) - 3.218876 * jax.random.uniform(keys[3], (IN, RANK), jnp.float32) ** shard_levels(keys[3], (IN, RANK), ((0, 32),), -0.2, 0.2)), 1.1302806607327298e-10, 2.8257016726485062e-09)
    step_count = jax.random.randint(keys[4], (1,), 1, 60).astype(jnp.int32)
    return dict(grads=grads, master=master, moment_one=moment_one, moment_two=moment_two, step_count=step_count)


def reference(grads, master, moment_one, moment_two, step_count):
    summed = lax.optimization_barrier(jnp.sum(grads, axis=(0, 1), dtype=jnp.float32))
    norm = jnp.sqrt(jnp.sum(summed * summed))
    clip = jnp.minimum(jnp.float32(1.0), 1.0 / (norm + 1e-06))
    gradient = clip * summed
    new_one = 0.9 * moment_one + 0.1 * gradient
    new_two = 0.999 * moment_two + 0.001 * gradient * gradient
    steps = step_count[0].astype(jnp.float32)
    first_fix = 1.0 - jnp.power(jnp.float32(0.9), steps)
    second_fix = 1.0 - jnp.power(jnp.float32(0.999), steps)
    update = new_one / first_fix / (jnp.sqrt(new_two / second_fix) + 1e-08)
    new_master = master - 0.01 * (update + 0.01 * master)
    return (new_master, new_one, new_two, new_master.astype(jnp.bfloat16))
```

```python
import functools

import jax
import jax.numpy as jnp
from jax import lax
from jax.experimental import pallas as pl
from jax.experimental.pallas import tpu as pltpu
from jax.sharding import PartitionSpec as P

MESH = pl.DeviceIdType.MESH
ROWS = 108
WIN = 112
LANES = 128
FAR, PLAIN, ACC = 0, 1, 2


def coded(value):
    top = jnp.maximum(jnp.max(jnp.abs(value), axis=0, keepdims=True), 1e-30)
    steps = jnp.round(value * (32767.0 / top))
    return steps.astype(jnp.int32).astype(jnp.int16), top * (1.0 / 32767.0)


def decoded(steps, scale):
    return steps.astype(jnp.int32).astype(jnp.float32) * scale


def kernel(
    grads, master, one, two, fixes,
    new_master, new_one, new_two, weights,
    own, sib, tx1, ts1, rx1, rs1, tx2, ts2, rx2, rs2, first, second,
    ztx, zts, zrx, zrs, total, nrm_y, nrm_x, nrm_z, wide, gathered,
    own_sem, d2d_s, d2d_r, s1, r1, ss1, sr1, s2, r2, ss2, sr2,
    zs, zr, zss, zsr, ns, nr, gs, gr, xs, xr, zns, znr, ws, wr, as1, ar1, as2, ar2, fs, fr,
):
    g = lax.axis_index("grp")
    s = lax.axis_index("shard")
    y, c = g // 2, g % 2
    x, z = s // 8, s % 8
    odd = z % 2
    part = z // 4
    owner = c == (z // 2) % 2

    def dev(x_=x, y_=y, z_=z, c_=c):
        return (y_ * 2 + c_, x_ * 8 + z_)

    def remote(src, dst, send, recv, device):
        return pltpu.make_async_remote_copy(
            src_ref=src, dst_ref=dst, send_sem=send, recv_sem=recv, device_id=device, device_id_type=MESH
        )

    def ring(a, n, k):
        return (a + k) % n

    sends = []

    def go(copy):
        copy.start()
        sends.append(copy)

    def rows(p, k, core):
        return pl.ds(pl.multiple_of(864 * ring(x, 4, k) + 432 * p + 216 * core, 8), 216)

    order = [(0, 2), (1, 0), (1, 1), (1, 2), (1, 3), (0, 1), (0, 3), (0, 0)]
    loads = {}
    for n, (p, k) in enumerate(order):
        loads[p, k] = pltpu.make_async_copy(grads.at[0, 0, rows(p, k, c)], own.at[p, k], own_sem.at[n])
        loads[p, k].start()

    barrier = pltpu.get_barrier_semaphore()
    partners = [dev(x_=ring(x, 4, k)) for k in (1, 2, 3)]
    partners += [dev(y_=ring(y, 4, k), c_=core) for k in (1, 2, 3) for core in (c, 1 - c)]
    partners += [dev(c_=1 - c)]
    partners += [dev(z_=ring(z, 8, k)) for k in range(1, 8)]
    for partner in partners:
        pl.semaphore_signal(barrier, inc=1, device_id=partner, device_id_type=MESH)
    pl.semaphore_wait(barrier, len(partners))

    pairs = {}
    for n, (p, k) in enumerate(order):
        pairs[p, k] = remote(
            grads.at[0, 0, rows(p, k, 1 - c)], sib.at[p, k], d2d_s.at[n], d2d_r.at[n], dev(c_=1 - c)
        )
        go(pairs[p, k])

    def chip_ready(p, k):
        loads[p, k].wait()
        pairs[p, k].wait_recv()

    def lanes(t):
        return pl.ds(pl.multiple_of(LANES * ring(y, 4, t), LANES), LANES)

    def chip_a(j, e, i):
        at = (0, j, pl.ds(104 * e, WIN), lanes(i))
        return own[at] + sib[at]

    def chip_b(j, e, i):
        at = (1, i, pl.ds(104 * e, WIN), lanes(j))
        return own[at] + sib[at]

    along_x = [dev(x_=ring(x, 4, 1)), dev(x_=ring(x, 4, 3))]
    along_y = [dev(y_=ring(y, 4, 1)), dev(y_=ring(y, 4, 3))]

    class Scatter:
        def __init__(self, value, many, ends, base, bufs, sems):
            self.value, self.many, self.ends, self.base = value, many, ends, base
            self.tx, self.ts, self.rx, self.rs = bufs
            self.sems = sems

        def slot(self, d, kind):
            return self.base * 6 + d * 3 + kind

        def copies(self, d, kind):
            n = self.slot(d, kind)
            send, recv, scale_send, scale_recv = self.sems
            return (
                remote(self.tx.at[n], self.rx.at[n], send.at[n], recv.at[n], self.ends[d]),
                remote(self.ts.at[n], self.rs.at[n], scale_send.at[n], scale_recv.at[n], self.ends[d]),
            )

        def each(self, body):
            if self.many == 1:
                body(0)
            else:
                lax.fori_loop(0, self.many, lambda i, _: (body(i), 0)[1], 0)

        def send(self, d, kind):
            n = self.slot(d, kind)
            chunk = 2 if kind == FAR else (1, 3)[d]
            half = 1 - d if kind == PLAIN else d

            def body(i):
                value = self.value(chunk, half, i)
                if kind == ACC:
                    m = self.slot(d, FAR)
                    value = value + decoded(self.rx[m, i], self.rs[m, i])
                self.tx[n, i], self.ts[n, i] = coded(value)

            self.each(body)
            for copy in self.copies(d, kind):
                go(copy)

        def arrive(self, d, kind):
            for copy in self.copies(d, kind):
                copy.wait_recv()

        def add_up(self, store):
            for e in (0, 1):
                m, n = self.slot(e, ACC), self.slot(1 - e, PLAIN)

                def body(i):
                    value = self.value(0, e, i) + decoded(self.rx[m, i], self.rs[m, i])
                    store(e, i, value + decoded(self.rx[n, i], self.rs[n, i]))

                self.each(body)

    bufs1, sems1 = (tx1, ts1, rx1, rs1), (s1, r1, ss1, sr1)
    bufs2, sems2 = (tx2, ts2, rx2, rs2), (s2, r2, ss2, sr2)
    sc_a = Scatter(chip_a, 4, along_x, 0, bufs1, sems1)
    sc_b = Scatter(chip_b, 4, along_y, 1, bufs1, sems1)

    chip_ready(0, 2)
    for d in (0, 1):
        sc_a.send(d, FAR)
    for k in range(4):
        chip_ready(1, k)
    for d in (0, 1):
        sc_b.send(d, FAR)
    chip_ready(0, 1)
    sc_a.send(0, PLAIN)
    chip_ready(0, 3)
    sc_a.send(1, PLAIN)
    for d in (0, 1):
        sc_b.send(d, PLAIN)
    for sc in (sc_a, sc_b):
        for d in (0, 1):
            sc.arrive(d, FAR)
            sc.send(d, ACC)
    chip_ready(0, 0)

    def keep_first(p):
        def store(e, i, value):
            first[p, e, i] = value

        return store

    sc2 = []
    for p, sc, ends in ((0, sc_a, along_y), (1, sc_b, along_x)):
        for kind in (PLAIN, ACC):
            for d in (0, 1):
                sc.arrive(d, kind)
        sc.add_up(keep_first(p))

        def value(j, e, i, p=p):
            return first[p, e, j]

        nxt = Scatter(value, 1, ends, p, bufs2, sems2)
        for kind in (FAR, PLAIN):
            for d in (0, 1):
                nxt.send(d, kind)
        sc2.append(nxt)
    for sc in sc2:
        for d in (0, 1):
            sc.arrive(d, FAR)
            sc.send(d, ACC)

    def z_copies(n, there, slot):
        device = dev(z_=there)
        return (
            remote(ztx.at[n], zrx.at[slot], zs.at[n], zr.at[slot], device),
            remote(zts.at[n], zrs.at[slot], zss.at[n], zsr.at[slot], device),
        )

    for p, sc in enumerate(sc2):
        for kind in (PLAIN, ACC):
            for d in (0, 1):
                sc.arrive(d, kind)

        def store(e, i, value, p=p):
            second[2 * p + e] = value

        sc.add_up(store)
        for e in (0, 1):
            n = 2 * p + e
            there = 4 * p + 2 * c + e
            ztx[n], zts[n] = coded(second[n])

            @pl.when(there != z)
            def _():
                for copy in z_copies(n, there, (z - there + 8) % 8):
                    copy.start()

    row = lax.broadcasted_iota(jnp.int32, (WIN, LANES), 0)

    @pl.when(owner)
    def _():
        value = second[2 * part + odd]
        for k in range(1, 8):
            for copy in z_copies(0, z, k):
                copy.wait_recv()
            value = value + decoded(zrx[k], zrs[k])
        value = jnp.where(odd == 1, pltpu.roll(value, WIN - 4, 0), value)
        value = jnp.where(row < ROWS, value, 0.0)
        total[0] = value
        nrm_y[0] = jnp.sum(value * value, axis=0, keepdims=True)

    group = [(k, core) for k in (1, 2, 3) for core in (0, 1)] + [(0, 1)]

    def norm_copy(n, k, core):
        device = dev(y_=ring(y, 4, k), c_=(c + core) % 2)
        return remote(nrm_y.at[0], nrm_y.at[(4 - k) % 4], ns.at[n], nr.at[(4 - k) % 4], device)

    def total_copy(n, k, core):
        device = dev(y_=ring(y, 4, k), c_=(c + core) % 2)
        return remote(total.at[0], total.at[(4 - k) % 4], gs.at[n], gr.at[(4 - k) % 4], device)

    @pl.when(owner)
    def _():
        for n, (k, core) in enumerate(group):
            norm_copy(n, k, core).start()
        for n, (k, core) in enumerate(group):
            total_copy(n, k, core).start()

    def in_turn(ref, here, size):
        value = ref[(size - here) % size]
        for k in range(1, size):
            value = value + ref[(k - here + size) % size]
        return value

    for k in (1, 2, 3):
        norm_copy(0, 4 - k, 0).wait_recv()

    @pl.when(jnp.logical_not(owner))
    def _():
        norm_copy(0, 0, 1).wait_recv()

    nrm_x[0] = in_turn(nrm_y, y, 4)
    x_norms = [
        remote(nrm_x.at[0], nrm_x.at[4 - k], xs.at[k], xr.at[4 - k], dev(x_=ring(x, 4, k))) for k in (1, 2, 3)
    ]
    for copy in x_norms:
        go(copy)
    for copy in x_norms:
        copy.wait_recv()
    nrm_z[0] = in_turn(nrm_x, x, 4)
    z_norms = [
        remote(nrm_z.at[0], nrm_z.at[8 - k], zns.at[k], znr.at[8 - k], dev(z_=ring(z, 8, k))) for k in range(1, 8)
    ]
    for copy in z_norms:
        go(copy)
    for copy in z_norms:
        copy.wait_recv()
    squares = jnp.sum(in_turn(nrm_z, z, 8), axis=1, keepdims=True)
    clip = jnp.minimum(1.0, 1.0 / (jnp.sqrt(squares) + 1e-06))
    first_fix, second_fix = fixes[0], fixes[1]

    def update(summed, at):
        gradient = clip * summed
        one_ = 0.9 * one[:, at] + 0.1 * gradient
        two_ = 0.999 * two[:, at] + 0.001 * gradient * gradient
        step = one_ / first_fix / (jnp.sqrt(two_ / second_fix) + 1e-08)
        return master[:, at] - 0.01 * (step + 0.01 * master[:, at]), one_, two_

    i_own, j_own = x + part * (y - x), y + part * (x - y)

    def weight_copy(n, there, p, e):
        at = gathered.at[c, p, i_own_of(p), e, j_own_of(p)]
        return remote(at, at, ws.at[n], wr.at[2 * p + e], dev(z_=there))

    def i_own_of(p):
        return x + p * (y - x)

    def j_own_of(p):
        return y + p * (x - y)

    @pl.when(owner)
    def _():
        wide[...] = jnp.zeros_like(wide)
        wide[0:ROWS] = update(total[0, 0:ROWS], lanes(0))[0]
        value = wide[...]
        value = jnp.where(odd == 1, pltpu.roll(value, 4, 0), value)
        gathered[c, part, i_own, odd, j_own] = value.astype(jnp.bfloat16)
        for k in range(1, 8):
            weight_copy(k, ring(z, 8, k), part, odd).start()

    for k in (1, 2, 3):
        total_copy(0, 4 - k, 0).wait_recv()

    @pl.when(jnp.logical_not(owner))
    def _():
        total_copy(0, 0, 1).wait_recv()

    for k in range(4):
        at = lanes(k)
        new_master[:, at], new_one[:, at], new_two[:, at] = update(total[k, 0:ROWS], at)

    for p in (0, 1):
        for e in (0, 1):
            there = 4 * p + 2 * c + e

            @pl.when(there != z)
            def _():
                weight_copy(0, z, p, e).wait_recv()

    class Gather:
        def __init__(self, slot, here, ends, base, sems):
            self.slot, self.here, self.ends, self.base, self.sems = slot, here, ends, base, sems

        def copy(self, d, kind, half, k):
            n = self.base * 6 + d * 3 + kind
            at = self.slot(half, ring(self.here, 4, k))
            return remote(at, at, self.sems[0].at[n], self.sems[1].at[n], self.ends[d])

        def start(self):
            for d in (0, 1):
                go(self.copy(d, 0, d, 0))
            for d in (0, 1):
                go(self.copy(d, 1, 1 - d, 0))

        def pass_on(self):
            for d in (0, 1):
                back = (3, 1)[d]
                self.copy(d, 0, d, back).wait_recv()
                go(self.copy(d, 2, d, back))

        def near(self, d):
            self.copy(d, 1, 1 - d, (3, 1)[d]).wait_recv()

        def far(self, d):
            self.copy(d, 2, d, 2).wait_recv()

    near = [
        Gather(lambda e, j: gathered.at[c, 0, x, e, j], y, along_y, 0, (as1, ar1)),
        Gather(lambda e, j: gathered.at[c, 1, y, e, j], x, along_x, 1, (as1, ar1)),
    ]
    wider = [
        Gather(lambda e, i: gathered.at[c, 0, i, e], x, along_x, 0, (as2, ar2)),
        Gather(lambda e, i: gathered.at[c, 1, i, e], y, along_y, 1, (as2, ar2)),
    ]
    for ga in near:
        ga.start()
    for ga in near:
        ga.pass_on()
    for p in (0, 1):
        for d in (0, 1):
            near[p].near(d)
            near[p].far(d)
        wider[p].start()

    def across(p, k, e, core=None):
        here = (x, y)[p]
        at = gathered.at[c, p, ring(here, 4, k), e]
        n = 8 * p + 2 * k + e
        return remote(at, at, fs.at[n], fr.at[n], dev(c_=1 - c))

    def place(p, k, t):
        here = (x, y)[p]
        i = ring(here, 4, k)
        pieces = []
        for core in (0, 1):
            low = gathered[core, p, i, 0, t].astype(jnp.float32)
            high = gathered[core, p, i, 1, t].astype(jnp.float32)
            mixed = jnp.where(row[0:8] < 4, low[104:112], high[0:8])
            pieces += [low[0:104], mixed, high[8:112]]
        value = jnp.concatenate(pieces, axis=0).astype(jnp.bfloat16)
        block, column = (i, t) if p == 0 else (t, i)
        weights[
            pl.ds(pl.multiple_of(864 * block + 432 * p, 16), 432),
            pl.ds(pl.multiple_of(LANES * column, LANES), LANES),
        ] = value

    for p in (0, 1):
        for e in (0, 1):
            go(across(p, 0, e))
    for p in (0, 1):
        wider[p].pass_on()
        for d in (0, 1):
            go(across(p, (3, 1)[d], d))
    for p in (0, 1):
        for d in (0, 1):
            wider[p].near(d)
            go(across(p, (3, 1)[d], 1 - d))

    def place_all(p, k):
        for e in (0, 1):
            across(p, k, e).wait_recv()
        lax.fori_loop(0, 4, lambda t, _: (place(p, k, t), 0)[1], 0)

    for p in (0, 1):
        place_all(p, 0)
    for p in (0, 1):
        for d in (0, 1):
            wider[p].far(d)
            go(across(p, 2, d))
    for k in (1, 3, 2):
        for p in (0, 1):
            place_all(p, k)

    for copy in sends:
        copy.wait_send()
    for p in (0, 1):
        for e in (0, 1):
            there = 4 * p + 2 * c + e

            @pl.when(there != z)
            def _():
                for copy in z_copies(2 * p + e, there, (z - there + 8) % 8):
                    copy.wait_send()

    @pl.when(owner)
    def _():
        for n, (k, core) in enumerate(group):
            norm_copy(n, k, core).wait_send()
            total_copy(n, k, core).wait_send()
        for k in range(1, 8):
            weight_copy(k, ring(z, 8, k), part, odd).wait_send()


def shards(grads, master, moment_one, moment_two, step_count):
    steps = step_count[0].astype(jnp.float32)
    fixes = jnp.stack([1.0 - jnp.power(jnp.float32(0.9), steps), 1.0 - jnp.power(jnp.float32(0.999), steps)])
    vmem = pl.BlockSpec(memory_space=pltpu.VMEM)
    f32, i16, bf16 = jnp.float32, jnp.int16, jnp.bfloat16
    dma = pltpu.SemaphoreType.DMA
    state = jax.ShapeDtypeStruct((ROWS, 512), f32)
    return pl.pallas_call(
        kernel,
        out_shape=(state, state, state, jax.ShapeDtypeStruct((3456, 512), bf16)),
        in_specs=[pl.BlockSpec(memory_space=pl.ANY), vmem, vmem, vmem, pl.BlockSpec(memory_space=pltpu.SMEM)],
        out_specs=(vmem, vmem, vmem, vmem),
        scratch_shapes=[
            pltpu.VMEM((2, 4, 216, 512), f32),
            pltpu.VMEM((2, 4, 216, 512), f32),
            pltpu.VMEM((12, 4, WIN, LANES), i16),
            pltpu.VMEM((12, 4, 1, LANES), f32),
            pltpu.VMEM((12, 4, WIN, LANES), i16),
            pltpu.VMEM((12, 4, 1, LANES), f32),
            pltpu.VMEM((12, 1, WIN, LANES), i16),
            pltpu.VMEM((12, 1, 1, LANES), f32),
            pltpu.VMEM((12, 1, WIN, LANES), i16),
            pltpu.VMEM((12, 1, 1, LANES), f32),
            pltpu.VMEM((2, 2, 4, WIN, LANES), f32),
            pltpu.VMEM((4, WIN, LANES), f32),
            pltpu.VMEM((4, WIN, LANES), i16),
            pltpu.VMEM((4, 1, LANES), f32),
            pltpu.VMEM((8, WIN, LANES), i16),
            pltpu.VMEM((8, 1, LANES), f32),
            pltpu.VMEM((4, WIN, LANES), f32),
            pltpu.VMEM((4, 1, LANES), f32),
            pltpu.VMEM((4, 1, LANES), f32),
            pltpu.VMEM((8, 1, LANES), f32),
            pltpu.VMEM((WIN, LANES), f32),
            pltpu.VMEM((2, 2, 4, 2, 4, WIN, LANES), bf16),
            dma((8,)), dma((8,)), dma((8,)),
            dma((12,)), dma((12,)), dma((12,)), dma((12,)),
            dma((12,)), dma((12,)), dma((12,)), dma((12,)),
            dma((4,)), dma((8,)), dma((4,)), dma((8,)),
            dma((7,)), dma((4,)), dma((7,)), dma((4,)),
            dma((4,)), dma((4,)), dma((8,)), dma((8,)),
            dma((8,)), dma((4,)),
            dma((12,)), dma((12,)), dma((12,)), dma((12,)),
            dma((16,)), dma((16,)),
        ],
        compiler_params=pltpu.CompilerParams(collective_id=0, has_side_effects=True, vmem_limit_bytes=60000 * 1024),
        name="step",
    )(grads, master, moment_one, moment_two, fixes)


def solution(mesh):
    in_specs = (P("grp", "shard", None, None), P("shard", None), P("shard", None), P("shard", None), P())
    out_specs = (P("shard", None), P("shard", None), P("shard", None), P())
    return jax.shard_map(shards, mesh=mesh, in_specs=in_specs, out_specs=out_specs, check_vma=False)
```

```python
import functools

import jax
import jax.numpy as jnp
from jax import lax
from jax.experimental import pallas as pl
from jax.experimental.pallas import tpu as pltpu
from jax.sharding import PartitionSpec as P

MESH = pl.DeviceIdType.MESH
ROWS = 108
WIN = 112
LANES = 128
FAR, PLAIN, ACC = 0, 1, 2


def coded(value):
    top = jnp.maximum(jnp.max(jnp.abs(value), axis=0, keepdims=True), 1e-30)
    steps = jnp.round(value * (32767.0 / top))
    return steps.astype(jnp.int32).astype(jnp.int16), top * (1.0 / 32767.0)


def decoded(steps, scale):
    return steps.astype(jnp.int32).astype(jnp.float32) * scale


def kernel(
    grads, master_, one_, two_, fixes,
    new_master, new_one, new_two, weights,
    master, one, two, state_sem, own_a, own_b, sib_a, sib_b,
    tx1, ts1, rx1, rs1, tx2, ts2, rx2, rs2, first, second,
    ztx, zts, zrx, zrs, total, plane, line, sum_of, wide, gathered,
    own_sem, d2d_s, d2d_r, s1, r1, ss1, sr1, s2, r2, ss2, sr2,
    zs, zr, zss, zsr, gs, gr, ps, pr, ls, lr, os, or_, ws, wr, as1, ar1, as2, ar2, fs, fr,
):
    g = lax.axis_index("grp")
    s = lax.axis_index("shard")
    y, c = g // 2, g % 2
    x, z = s // 8, s % 8
    odd = z % 2
    part = z // 4

    def core_of(z_):
        return (z_ // 2) % 2

    owner = c == core_of(z)

    def dev(x_=x, y_=y, z_=z, c_=c):
        return (y_ * 2 + c_, x_ * 8 + z_)

    def remote(src, dst, send, recv, device):
        return pltpu.make_async_remote_copy(
            src_ref=src, dst_ref=dst, send_sem=send, recv_sem=recv, device_id=device, device_id_type=MESH
        )

    def ring(a, n, k):
        return (a + k) % n

    sends = []

    def go(copy):
        copy.start()
        sends.append(copy)

    def lanes(t):
        return pl.ds(pl.multiple_of(LANES * ring(y, 4, t), LANES), LANES)

    def chunk(p, j, core):
        if p == 0:
            return grads.at[ring(x, 4, j), pl.ds(pl.multiple_of(216 * core, 8), 216)]
        return grads.at[:, pl.ds(pl.multiple_of(432 + 216 * core, 8), 216), lanes(j)]

    own, sib = (own_a, own_b), (sib_a, sib_b)
    order = [(0, 2), (1, 2), (0, 1), (0, 3), (1, 1), (1, 3), (0, 0), (1, 0)]
    loads = {}
    for n, (p, j) in enumerate(order):
        loads[p, j] = pltpu.make_async_copy(chunk(p, j, c), own[p].at[j], own_sem.at[n])
        loads[p, j].start()
    state = [
        pltpu.make_async_copy(src, dst, state_sem.at[n])
        for n, (src, dst) in enumerate(((master_, master), (one_, one), (two_, two)))
    ]
    for copy in state:
        copy.start()

    plane_of = [(i, k) for i in range(4) for k in range(4) if i or k]
    barrier = pltpu.get_barrier_semaphore()
    partners = [dev(c_=1 - c)]
    partners += [dev(x_=ring(x, 4, i), y_=ring(y, 4, k)) for i, k in plane_of]
    partners += [dev(z_=ring(z, 8, k), c_=core) for k in range(1, 8) for core in (c, 1 - c)]
    for partner in partners:
        pl.semaphore_signal(barrier, inc=1, device_id=partner, device_id_type=MESH)
    pl.semaphore_wait(barrier, len(partners))

    pairs = {}
    for n, (p, j) in enumerate(order):
        pairs[p, j] = remote(chunk(p, j, 1 - c), sib[p].at[j], d2d_s.at[n], d2d_r.at[n], dev(c_=1 - c))
        go(pairs[p, j])

    def chip_ready(p, j):
        loads[p, j].wait()
        pairs[p, j].wait_recv()

    def chip_a(j, e, i):
        at = (j, pl.ds(104 * e, WIN), lanes(i))
        return own_a[at] + sib_a[at]

    def chip_b(j, e, i):
        at = (j, ring(x, 4, i), pl.ds(104 * e, WIN))
        return own_b[at] + sib_b[at]

    along_x = [dev(x_=ring(x, 4, 1)), dev(x_=ring(x, 4, 3))]
    along_y = [dev(y_=ring(y, 4, 1)), dev(y_=ring(y, 4, 3))]

    class Scatter:
        def __init__(self, value, many, ends, base, bufs, sems):
            self.value, self.many, self.ends, self.base = value, many, ends, base
            self.tx, self.ts, self.rx, self.rs = bufs
            self.sems = sems

        def slot(self, d, kind, i):
            return (self.base * 6 + d * 3 + kind) * self.many + i

        def copies(self, d, kind, i):
            n = self.slot(d, kind, i)
            send, recv, scale_send, scale_recv = self.sems
            return (
                remote(self.tx.at[n], self.rx.at[n], send.at[n], recv.at[n], self.ends[d]),
                remote(self.ts.at[n], self.rs.at[n], scale_send.at[n], scale_recv.at[n], self.ends[d]),
            )

        def arrived(self, d, kind, i):
            n = self.slot(d, kind, i)
            for copy in self.copies(d, kind, i):
                copy.wait_recv()
            return decoded(self.rx[n], self.rs[n])

        def send(self, d, kind, i):
            n = self.slot(d, kind, i)
            j = 2 if kind == FAR else (1, 3)[d]
            half = 1 - d if kind == PLAIN else d
            value = self.value(j, half, i)
            if kind == ACC:
                value = value + self.arrived(d, FAR, i)
            self.tx[n], self.ts[n] = coded(value)
            for copy in self.copies(d, kind, i):
                go(copy)

        def result(self, e, i):
            return self.value(0, e, i) + self.arrived(1 - e, PLAIN, i) + self.arrived(e, ACC, i)

    bufs1, sems1 = (tx1, ts1, rx1, rs1), (s1, r1, ss1, sr1)
    bufs2, sems2 = (tx2, ts2, rx2, rs2), (s2, r2, ss2, sr2)
    sc = [Scatter(chip_a, 4, along_x, 0, bufs1, sems1), Scatter(chip_b, 4, along_y, 1, bufs1, sems1)]
    nxt = [
        Scatter(lambda j, e, i: first[0, e, j], 1, along_y, 0, bufs2, sems2),
        Scatter(lambda j, e, i: first[1, e, j], 1, along_x, 1, bufs2, sems2),
    ]
    turns = (2, 1, 3, 0)

    for p in (0, 1):
        chip_ready(p, 2)
        for i in turns:
            for d in (0, 1):
                sc[p].send(d, FAR, i)
    for p in (0, 1):
        chip_ready(p, 1)
        chip_ready(p, 3)
        for d in (0, 1):
            sc[p].send(d, PLAIN, 2)
    for i in turns:
        for p in (0, 1):
            for d in (0, 1):
                if i != 2:
                    sc[p].send(d, PLAIN, i)
                sc[p].send(d, ACC, i)
    for p in (0, 1):
        chip_ready(p, 0)

    for i in turns:
        for p in (0, 1):
            for e in (0, 1):
                first[p, e, i] = sc[p].result(e, i)
            if i == 2:
                for d in (0, 1):
                    nxt[p].send(d, FAR, 0)
            elif i:
                nxt[p].send((i - 1) // 2, PLAIN, 0)
    for p in (0, 1):
        for d in (0, 1):
            nxt[p].send(d, ACC, 0)

    def z_copies(n, there, slot):
        device = dev(z_=there)
        return (
            remote(ztx.at[n], zrx.at[slot], zs.at[n], zr.at[slot], device),
            remote(zts.at[n], zrs.at[slot], zss.at[n], zsr.at[slot], device),
        )

    for p in (0, 1):
        for e in (0, 1):
            n = 2 * p + e
            there = 4 * p + 2 * c + e
            value = nxt[p].result(e, 0)
            second[n] = value
            ztx[n], zts[n] = coded(value)

            @pl.when(there != z)
            def _():
                for copy in z_copies(n, there, (z - there + 8) % 8):
                    copy.start()

    row = lax.broadcasted_iota(jnp.int32, (WIN, LANES), 0)

    def plane_copy(i, k):
        back = 4 * ((4 - i) % 4) + (4 - k) % 4
        return remote(plane.at[0], plane.at[back], ps.at[4 * i + k], pr.at[back], dev(x_=ring(x, 4, i), y_=ring(y, 4, k)))

    def line_copy(k):
        there = ring(z, 8, k)
        return remote(line.at[0], line.at[8 - k], ls.at[k], lr.at[8 - k], dev(z_=there, c_=core_of(there)))

    def sum_copy():
        return remote(sum_of, sum_of, os.at[0], or_.at[0], dev(c_=1 - c))

    def total_copy(k):
        return remote(total.at[0], total.at[(4 - k) % 4], gs.at[k], gr.at[(4 - k) % 4], dev(y_=ring(y, 4, k)))

    def total_across(k):
        return remote(total.at[k], total.at[k], gs.at[4 + k], gr.at[4 + k], dev(c_=1 - c))

    def i_own(p):
        return x + p * (y - x)

    def j_own(p):
        return y + p * (x - y)

    def weight_copy(n, there, p, e):
        at = gathered.at[c, p, i_own(p), e, j_own(p)]
        return remote(at, at, ws.at[n], wr.at[2 * p + e], dev(z_=there))

    first_fix, second_fix = fixes[0], fixes[1]
    for copy in state:
        copy.wait()

    def update(summed, at):
        squares = jnp.sum(sum_of[...], axis=1, keepdims=True)
        clip = jnp.minimum(1.0, 1.0 / (jnp.sqrt(squares) + 1e-06))
        gradient = clip * summed
        first_moment = 0.9 * one[:, at] + 0.1 * gradient
        second_moment = 0.999 * two[:, at] + 0.001 * gradient * gradient
        step = first_moment / first_fix / (jnp.sqrt(second_moment / second_fix) + 1e-08)
        return master[:, at] - 0.01 * (step + 0.01 * master[:, at]), first_moment, second_moment

    @pl.when(owner)
    def _():
        value = second[2 * part + odd]
        for k in range(1, 8):
            for copy in z_copies(0, z, k):
                copy.wait_recv()
            value = value + decoded(zrx[k], zrs[k])
        value = jnp.where(odd == 1, pltpu.roll(value, WIN - 4, 0), value)
        value = jnp.where(row < ROWS, value, 0.0)
        total[0] = value
        plane[0] = jnp.sum(value * value, axis=0, keepdims=True)
        for i, k in plane_of:
            plane_copy(i, k).start()
        for i, k in plane_of:
            plane_copy(i, k).wait_recv()
        value = jnp.zeros((1, LANES), jnp.float32)
        for i in range(4):
            for k in range(4):
                value = value + plane[4 * ring(i, 4, 4 - x) + ring(k, 4, 4 - y)]
        line[0] = value
        for k in range(1, 8):
            line_copy(k).start()
        for k in range(1, 8):
            line_copy(k).wait_recv()
        value = line[(8 - z) % 8]
        for k in range(1, 8):
            value = value + line[(k + 8 - z) % 8]
        sum_of[...] = value
        wide[...] = jnp.zeros_like(wide)
        wide[0:ROWS] = update(total[0, 0:ROWS], lanes(0))[0]
        value = wide[...]
        value = jnp.where(odd == 1, pltpu.roll(value, 4, 0), value)
        gathered[c, part, i_own(part), odd, j_own(part)] = value.astype(jnp.bfloat16)
        for k in (4, 3, 5, 2, 6, 1, 7):
            weight_copy(k, ring(z, 8, k), part, odd).start()
        sum_copy().start()
        for k in (1, 2, 3):
            total_copy(k).start()

    class Gather:
        def __init__(self, slot, here, ends, base, sems, many=1):
            self.slot, self.here, self.ends, self.base, self.sems = slot, here, ends, base, sems
            self.many = many

        def copy(self, d, kind, half, k, j=0):
            n = (self.base * 6 + d * 3 + kind) * self.many + j
            at = self.slot(half, ring(self.here, 4, k), j)
            return remote(at, at, self.sems[0].at[n], self.sems[1].at[n], self.ends[d])

        def start(self, half, j=0):
            for d in (half, 1 - half):
                go(self.copy(d, 0 if half == d else 1, half, 0, j))

        def pass_on(self, d, j=0):
            back = (3, 1)[d]
            self.copy(d, 0, d, back, j).wait_recv()
            go(self.copy(d, 2, d, back, j))

        def near(self, d, j=0):
            self.copy(d, 1, 1 - d, (3, 1)[d], j).wait_recv()

        def far(self, d, j=0):
            self.copy(d, 2, d, 2, j).wait_recv()

    near = [
        Gather(lambda e, k, j: gathered.at[c, 0, x, e, k], y, along_y, 0, (as1, ar1)),
        Gather(lambda e, k, j: gathered.at[c, 1, y, e, k], x, along_x, 1, (as1, ar1)),
    ]
    wider = [
        Gather(lambda e, k, j: gathered.at[c, 0, k, e, ring(y, 4, j)], x, along_x, 0, (as2, ar2), 4),
        Gather(lambda e, k, j: gathered.at[c, 1, k, e, ring(x, 4, j)], y, along_y, 1, (as2, ar2), 4),
    ]

    def across(p, k, e):
        at = gathered.at[c, p, ring((x, y)[p], 4, k), e]
        n = 8 * p + 2 * k + e
        return remote(at, at, fs.at[n], fr.at[n], dev(c_=1 - c))

    def place(p, k, t):
        i = ring((x, y)[p], 4, k)
        pieces = []
        for core in (0, 1):
            low = gathered[core, p, i, 0, t].astype(jnp.float32)
            high = gathered[core, p, i, 1, t].astype(jnp.float32)
            mixed = jnp.where(row[0:8] < 4, low[104:112], high[0:8])
            pieces += [low[0:104], mixed, high[8:112]]
        value = jnp.concatenate(pieces, axis=0).astype(jnp.bfloat16)
        block, column = (i, t) if p == 0 else (t, i)
        weights[
            pl.ds(pl.multiple_of(864 * block + 432 * p, 16), 432),
            pl.ds(pl.multiple_of(LANES * column, LANES), LANES),
        ] = value

    def place_all(p, k):
        for e in (0, 1):
            across(p, k, e).wait_recv()
        lax.fori_loop(0, 4, lambda t, _: (place(p, k, t), 0)[1], 0)

    both = [(p, e) for p in (0, 1) for e in (0, 1)]
    for p, e in both:
        there = 4 * p + 2 * c + e

        @pl.when(there != z)
        def _():
            weight_copy(0, z, p, e).wait_recv()

        near[p].start(e)
    for p, e in both:
        wider[p].start(e, 0)
    for p, d in both:
        near[p].pass_on(d)
        wider[p].start(d, (3, 1)[d])
    for p, d in both:
        near[p].near(d)
        wider[p].start(1 - d, (3, 1)[d])
    for p, d in both:
        wider[p].pass_on(d, 0)
    for p, d in both:
        near[p].far(d)
        wider[p].start(d, 2)
    for p, e in both:
        go(across(p, 0, e))

    @pl.when(owner)
    def _():
        for k in (1, 2, 3):
            total_copy(4 - k).wait_recv()
        for k in range(4):
            total_across(k).start()

    @pl.when(jnp.logical_not(owner))
    def _():
        sum_copy().wait_recv()
        for k in range(4):
            total_across(k).wait_recv()

    for k in range(4):
        at = lanes(k)
        new_master[:, at], new_one[:, at], new_two[:, at] = update(total[k, 0:ROWS], at)

    for j in (3, 1):
        for p, d in both:
            wider[p].pass_on(d, j)
    for p in (0, 1):
        place_all(p, 0)
    for p, d in both:
        wider[p].pass_on(d, 2)
        go(across(p, (3, 1)[d], d))
    for p, d in both:
        for j in (0, 3, 1, 2):
            wider[p].near(d, j)
        go(across(p, (3, 1)[d], 1 - d))
    for p, d in both:
        for j in (0, 3, 1, 2):
            wider[p].far(d, j)
        go(across(p, 2, d))
    for k in (1, 3, 2):
        for p in (0, 1):
            place_all(p, k)

    for copy in sends:
        copy.wait_send()
    for p, e in both:
        there = 4 * p + 2 * c + e

        @pl.when(there != z)
        def _():
            for copy in z_copies(2 * p + e, there, (z - there + 8) % 8):
                copy.wait_send()

    @pl.when(owner)
    def _():
        for i, k in plane_of:
            plane_copy(i, k).wait_send()
        for k in range(1, 8):
            line_copy(k).wait_send()
            weight_copy(k, ring(z, 8, k), part, odd).wait_send()
        sum_copy().wait_send()
        for k in (1, 2, 3):
            total_copy(k).wait_send()
        for k in range(4):
            total_across(k).wait_send()


def finish(*refs):
    sources, results, sems = refs[:4], refs[4:8], refs[8]
    copies = [pltpu.make_async_copy(src, dst, sems.at[n]) for n, (src, dst) in enumerate(zip(sources, results))]
    for copy in copies[::-1]:
        copy.start()
    for copy in copies:
        copy.wait()


def shards(grads, master, moment_one, moment_two, step_count):
    steps = step_count[0].astype(jnp.float32)
    fixes = jnp.stack([1.0 - jnp.power(jnp.float32(0.9), steps), 1.0 - jnp.power(jnp.float32(0.999), steps)])
    vmem = pl.BlockSpec(memory_space=pltpu.VMEM)
    f32, i16, bf16 = jnp.float32, jnp.int16, jnp.bfloat16
    dma = pltpu.SemaphoreType.DMA
    state = jax.ShapeDtypeStruct((ROWS, 512), f32)
    results = (state, state, state, jax.ShapeDtypeStruct((3456, 512), bf16))
    hbm, anywhere = pl.BlockSpec(memory_space=pltpu.HBM), pl.BlockSpec(memory_space=pl.ANY)
    grads = grads.reshape(4, 864, 512)
    grads, master, moment_one, moment_two = (
        pltpu.with_memory_space_constraint(value, pltpu.HBM) for value in (grads, master, moment_one, moment_two)
    )
    made = pl.pallas_call(
        kernel,
        out_shape=results,
        in_specs=[hbm, hbm, hbm, hbm, pl.BlockSpec(memory_space=pltpu.SMEM)],
        out_specs=(vmem, vmem, vmem, vmem),
        scratch_shapes=[
            pltpu.VMEM((ROWS, 512), f32),
            pltpu.VMEM((ROWS, 512), f32),
            pltpu.VMEM((ROWS, 512), f32),
            dma((3,)),
            pltpu.VMEM((4, 216, 512), f32),
            pltpu.VMEM((4, 4, 216, LANES), f32),
            pltpu.VMEM((4, 216, 512), f32),
            pltpu.VMEM((4, 4, 216, LANES), f32),
            pltpu.VMEM((48, WIN, LANES), i16),
            pltpu.VMEM((48, 1, LANES), f32),
            pltpu.VMEM((48, WIN, LANES), i16),
            pltpu.VMEM((48, 1, LANES), f32),
            pltpu.VMEM((12, WIN, LANES), i16),
            pltpu.VMEM((12, 1, LANES), f32),
            pltpu.VMEM((12, WIN, LANES), i16),
            pltpu.VMEM((12, 1, LANES), f32),
            pltpu.VMEM((2, 2, 4, WIN, LANES), f32),
            pltpu.VMEM((4, WIN, LANES), f32),
            pltpu.VMEM((4, WIN, LANES), i16),
            pltpu.VMEM((4, 1, LANES), f32),
            pltpu.VMEM((8, WIN, LANES), i16),
            pltpu.VMEM((8, 1, LANES), f32),
            pltpu.VMEM((4, WIN, LANES), f32),
            pltpu.VMEM((16, 1, LANES), f32),
            pltpu.VMEM((8, 1, LANES), f32),
            pltpu.VMEM((1, LANES), f32),
            pltpu.VMEM((WIN, LANES), f32),
            pltpu.VMEM((2, 2, 4, 2, 4, WIN, LANES), bf16),
            dma((8,)), dma((8,)), dma((8,)),
            dma((48,)), dma((48,)), dma((48,)), dma((48,)),
            dma((12,)), dma((12,)), dma((12,)), dma((12,)),
            dma((4,)), dma((8,)), dma((4,)), dma((8,)),
            dma((8,)), dma((8,)),
            dma((16,)), dma((16,)), dma((8,)), dma((8,)), dma((1,)), dma((1,)),
            dma((8,)), dma((4,)),
            dma((12,)), dma((12,)), dma((48,)), dma((48,)),
            dma((16,)), dma((16,)),
        ],
        compiler_params=pltpu.CompilerParams(collective_id=0, has_side_effects=True, vmem_limit_bytes=24 * 2**20),
        name="step",
    )(grads, master, moment_one, moment_two, fixes)
    return pl.pallas_call(
        finish,
        out_shape=results,
        in_specs=[anywhere] * 4,
        out_specs=(hbm, hbm, hbm, hbm),
        scratch_shapes=[dma((4,))],
        compiler_params=pltpu.CompilerParams(vmem_limit_bytes=2**20),
        name="finish",
    )(*made)


def solution(mesh):
    in_specs = (P("grp", "shard", None, None), P("shard", None), P("shard", None), P("shard", None), P())
    out_specs = (P("shard", None), P("shard", None), P("shard", None), P())
    return jax.shard_map(shards, mesh=mesh, in_specs=in_specs, out_specs=out_specs, check_vma=False)
```
